32 devices in a mesh: wide: 16 (over z, x, core), narrow: 2 (over y).
Axes of the slice: x: 2, y: 2, z: 4, core: 2. Of those that a mesh axis runs over, the one named last changes fastest.
Arguments:
- right_side: float32 [3, 256, 32, 128], P(None, 'wide', 'narrow'), may hold values from -8 to 8
- occupancy: int32 [256, 32, 128], P('wide', 'narrow'), may hold values from 0 to 1, as said below
- region: int32 [256, 32, 128], P('wide', 'narrow'), may hold values from 0 to 3
- coarse_inverse: float32 [384, 384], P(('wide', 'narrow')), as said below
Outputs:
- solution_field: float32 [3, 256, 32, 128], P(None, 'wide', 'narrow')
- residual: float32 [3, 256, 32, 128], P(None, 'wide', 'narrow')
The draws below stay inside these ranges and needn't reach their ends.
Inputs may be any that keep to these rules, and one draw needn't show every extreme that they name: `occupancy`: each subdomain has its own bone fraction between 0.15 and 0.9. `coarse_inverse`: symmetric positive definite.
All inputs are finite; a program needn't handle non-finite values.
Results may differ from the reference program's by a relative error of at most 0.00021.
Values sent between devices are 32-bit elements; how exact they have to be, the bound alone decides.
A program may use at most 64 MiB of HBM per device.

```python
import jax
import jax.numpy as jnp
from jax import lax

CX = 16
CY = 16
CZ = 128
NREG = 4
ITERS = 2
NX = 256
NY = 32
NZ = 128
NCOARSE = 384
N_WIDE = 16
N_NARROW = 2


def draw_occupancy(key, part):
    first, second = jax.random.split(key)
    wide_count = NX // CX
    narrow_count = NY // CY
    percent = jax.random.randint(first, (wide_count, narrow_count), 15, 91)
    level = jnp.repeat(jnp.repeat(percent, CX, axis=0), CY, axis=1)[:, :, None]
    bits = jax.random.randint(second, (NX, NY, NZ), 0, 100)
    return (bits < level).astype(jnp.int32)


def draw_coarse_inverse(key, part):
    first, second = jax.random.split(jax.random.fold_in(key, 7), 2)
    count = NCOARSE
    factor = jax.random.normal(first, (count, count), jnp.float32)
    gram = jnp.dot(factor, factor.T) / count
    gram = 0.5 * (gram + gram.T)
    diag = jax.random.uniform(second, (count,), jnp.float32, 0.5, 1.5)
    whole = gram + jnp.diag(diag)
    scale = 0.05 * jnp.sqrt(jnp.float32(NREG) / jnp.float32(CX * CY * CZ))
    return (whole * scale).astype(jnp.float32)


def with_ends(values, rng, low, top_value):
    dims = values.shape
    spot = [jax.random.randint(jax.random.fold_in(rng, axis), (), 0, dims[axis]) for axis in range(len(dims))]
    values = values.at[tuple(spot)].set(low)
    longest = dims.index(max(dims))
    spot[longest] = (spot[longest] + 1) % dims[longest]
    return values.at[tuple(spot)].set(top_value)


def level_of(stream_key, extent, shards, smallest, largest):
    factor_of = 1.0
    for dim, parts in shards:
        steps = jax.random.uniform(jax.random.fold_in(jax.random.fold_in(stream_key, 6), dim), (parts,), jnp.float32, smallest / len(shards), largest / len(shards))
        factor_of = factor_of * jnp.repeat(jnp.exp(steps), extent[dim] // parts).reshape((-1,) + (1,) * (len(extent) - 1 - dim))
    return factor_of


def centred(rng, shape, width, most, pieces=(), dtype=jnp.bfloat16):
    values = jax.random.normal(rng, shape, jnp.float32) * width
    if len(pieces) > 0:
        values = level_of(rng, shape, pieces, -0.22, 0.18) * values
    return jnp.clip(values, min=-most, max=most).astype(dtype)


def setup_inputs(seed: int = 0) -> dict:
    key_of = jax.random.split(jax.random.key(seed), 5)
    return {
        "right_side": centred(key_of[0], (3, NX, NY, NZ), 1.0, 8.0, ((1, 16), (2, 2)), jnp.float32),
        "occupancy": draw_occupancy(jax.random.fold_in(key_of[4], 71), 0),
        "region": with_ends(jax.random.randint(key_of[2], (NX, NY, NZ), 0, NREG), jax.random.fold_in(key_of[2], 1), 0, NREG - 1).astype(jnp.int32),
        "coarse_inverse": draw_coarse_inverse(jax.random.fold_in(key_of[4], 71), 0),
    }


bone_stiff = 1.0
soft_stiff = 0.1


def neighbours(padded):
    return [padded[..., 2:, 1:-1, 1:-1], padded[..., :-2, 1:-1, 1:-1],
            padded[..., 1:-1, 2:, 1:-1], padded[..., 1:-1, :-2, 1:-1],
            padded[..., 1:-1, 1:-1, 2:], padded[..., 1:-1, 1:-1, :-2]]


def reference(right_side, occupancy, region, coarse_inverse):
    stiff = soft_stiff + (bone_stiff - soft_stiff) * occupancy.astype(jnp.float32)
    faces = [0.5 * (stiff + other) for other in neighbours(jnp.pad(stiff, 1))]
    diagonal = sum(faces) + 0.5 * stiff
    wide_count = N_WIDE
    narrow_count = N_NARROW

    def operate(field):
        padded = jnp.pad(field, ((0, 0), (1, 1), (1, 1), (1, 1)))
        result = 0.25 * stiff * (field + jnp.sum(field, axis=0, keepdims=True))
        for face, other in zip(faces, neighbours(padded)):
            result = result + face * (field - other)
        return result

    selects = [(region == g).astype(jnp.float32).reshape(wide_count, CX, narrow_count, CY, CZ) for g in range(NREG)]

    def precondition(resid):
        blocks = resid.reshape(3, wide_count, CX, narrow_count, CY, CZ)
        coarse = jnp.stack([jnp.einsum('cwxnyz,wxnyz->wnc', blocks, s, precision=lax.Precision.HIGHEST) for s in selects], axis=2).reshape(-1)
        answer = jnp.dot(coarse_inverse, coarse, precision=lax.Precision.HIGHEST).reshape(wide_count, narrow_count, NREG, 3)
        spread = jnp.zeros_like(blocks)
        for g in range(NREG):
            spread = spread + jnp.einsum('wxnyz,wnc->cwxnyz', selects[g], answer[:, :, g, :], precision=lax.Precision.HIGHEST)
        return resid / diagonal + spread.reshape(resid.shape)

    solution = jnp.zeros_like(right_side)
    resid = right_side
    precond = precondition(resid)
    direction = precond
    rz_now = jnp.sum(resid * precond)
    for step in range(ITERS):
        image = operate(direction)
        alpha = rz_now / jnp.sum(direction * image)
        solution = solution + alpha * direction
        resid = resid - alpha * image
        precond = precondition(resid)
        rz_next = jnp.sum(resid * precond)
        direction = precond + (rz_next / rz_now) * direction
        rz_now = rz_next
    return solution, resid
```

```python
import functools

import jax
import jax.numpy as jnp
from jax import lax
from jax.experimental import pallas as pl
from jax.experimental.pallas import tpu as pltpu
from jax.sharding import PartitionSpec as P

LANES = 128
SUB = 8
MESH = pl.DeviceIdType.MESH
bone_stiff = 1.0
soft_stiff = 0.1


def kernel(nw, nn, r_hbm, occ_hbm, reg_hbm, ci_hbm, x_out, res_out,
           r_v, occ_v, reg_v, c_v, k_p, kx, kym, kyp, kzm, kzp, dg, invd,
           z_p, y_v, v_p, az_v, zy, vy,
           ix_in, iy_send, iy_in, c_in, wx_send, wx_in, wy_send, wy_in,
           row_send, rows, load_sem, hs_send, hs_recv, ag_send, ag_recv):
    X, Y, Z = occ_v.shape
    ncr, NC = c_v.shape
    G = ncr // 3
    ND = nw * nn
    wi = lax.axis_index("wide")
    ni = lax.axis_index("narrow")
    me = wi * nn + ni
    f32 = jnp.float32

    loads = [pltpu.make_async_copy(s, d, load_sem.at[i]) for i, (s, d) in enumerate(
        ((occ_hbm, occ_v), (reg_hbm, reg_v), (r_hbm, r_v), (ci_hbm, c_v)))]
    for l in loads:
        l.start()

    def peer(i):
        t = lax.rem(me + i, ND)
        return (t // nn, lax.rem(t, nn))

    barrier = pltpu.get_barrier_semaphore()

    def greet(i, _):
        pl.semaphore_signal(barrier, inc=1, device_id=peer(i), device_id_type=MESH)
        return 0

    lax.fori_loop(1, ND, greet, 0, unroll=ND <= 64)

    has = (wi > 0, wi < nw - 1, ni > 0, ni < nn - 1)
    to = ((wi - 1, ni), (wi + 1, ni), (wi, ni - 1), (wi, ni + 1))

    for d in range(4):
        @pl.when(jnp.logical_not(has[d]))
        def _():
            c_in[d] = jnp.zeros((ncr, NC), f32)
            for p in range(2):
                if d < 2:
                    wx_in[p, d] = jnp.zeros((3, Y, Z), f32)
                else:
                    wy_in[p, d - 2] = jnp.zeros((3, X, Z), f32)
            if d < 2:
                ix_in[d] = jnp.zeros((2, Y, Z), jnp.int32)
            else:
                iy_in[d - 2] = jnp.zeros((2, X, Z), jnp.int32)

    loads[0].wait()
    loads[1].wait()

    def pack_ints(x, _):
        iy_send[0, 0, pl.ds(x, 1), :] = occ_v[x, 0:1, :]
        iy_send[1, 0, pl.ds(x, 1), :] = occ_v[x, Y - 1:Y, :]
        iy_send[0, 1, pl.ds(x, 1), :] = reg_v[x, 0:1, :]
        iy_send[1, 1, pl.ds(x, 1), :] = reg_v[x, Y - 1:Y, :]
        return 0

    lax.fori_loop(0, X, pack_ints, 0)

    def fold(a):
        return jnp.sum(a.reshape(Y // SUB, SUB, Z), axis=0)

    def zero_acc(n):
        return tuple(jnp.zeros((SUB, Z), f32) for _ in range(n))

    def add_rc(acc, reg, u):
        out = list(acc)
        for g in range(G):
            m = reg == g
            for c in range(3):
                out[g * 3 + c] = acc[g * 3 + c] + fold(jnp.where(m, u[c], 0.0))
        return tuple(out)

    base = (me * ncr) % LANES

    def make_row(p, acc, first):
        a = jnp.concatenate([jnp.sum(b, axis=0, keepdims=True) for b in acc], axis=0)
        col = jnp.sum(a, axis=1, keepdims=True)
        n = len(acc)
        k = lax.broadcasted_iota(jnp.int32, (n, LANES), 0)
        lane = lax.broadcasted_iota(jnp.int32, (n, LANES), 1)
        target = (base + first + k) & (LANES - 1)
        row = jnp.sum(jnp.where(lane == target, col, 0.0), axis=0, keepdims=True)
        row_send[p, 0:1, :] = row
        rows[p, pl.ds(me, 1), :] = row

    def gather_start(p):
        def send(i, _):
            pltpu.make_async_remote_copy(
                src_ref=row_send.at[p, pl.ds(0, 1)], dst_ref=rows.at[p, pl.ds(me, 1)],
                send_sem=ag_send.at[p], recv_sem=ag_recv.at[p],
                device_id=peer(i), device_id_type=MESH).start()
            return 0
        lax.fori_loop(1, ND, send, 0, unroll=ND <= 64)

    def gather_wait(p, sem):
        part = rows.at[p, pl.ds(0, ND - 1)]
        pltpu.make_async_copy(part, part, sem.at[p]).wait()

    def coarse_vector(p):
        tiles = []
        for t in range(NC // LANES):
            lo = (LANES * t) // ncr // SUB * SUB
            hi = min(ND, -(-(-(-(LANES * (t + 1)) // ncr)) // SUB) * SUB)
            d = lax.broadcasted_iota(jnp.int32, (hi - lo, LANES), 0) + lo
            j = lax.broadcasted_iota(jnp.int32, (hi - lo, LANES), 1) + LANES * t
            m = (j >= d * ncr) & (j < d * ncr + ncr)
            tiles.append(jnp.sum(jnp.where(m, rows[p, lo:hi, :], 0.0), axis=0, keepdims=True))
        return tiles

    def total(p, s):
        d = lax.broadcasted_iota(jnp.int32, (ND, LANES), 0)
        lane = lax.broadcasted_iota(jnp.int32, (ND, LANES), 1)
        m = lane == ((d * ncr + ncr + s) & (LANES - 1))
        v = jnp.sum(jnp.where(m, rows[p], 0.0), axis=0, keepdims=True)
        return jnp.sum(v, axis=1, keepdims=True)

    def answers(tiles, ref):
        s = ref[:, 0:LANES] * tiles[0]
        for t in range(1, len(tiles)):
            s = s + ref[:, t * LANES:(t + 1) * LANES] * tiles[t]
        q = jnp.sum(s, axis=1, keepdims=True)
        return [q[i:i + 1, :] for i in range(ncr)]

    def spread(reg, q):
        masks = [reg == g for g in range(G)]
        out = []
        for c in range(3):
            s = jnp.zeros(reg.shape, f32)
            for g in range(G):
                s = jnp.where(masks[g], q[g * 3 + c], s)
            out.append(s)
        return out

    def halo(slot, d, src, dst):
        return pltpu.make_async_remote_copy(
            src_ref=src, dst_ref=dst, send_sem=hs_send.at[slot, d],
            recv_sem=hs_recv.at[slot, d ^ 1], device_id=to[d], device_id_type=MESH)

    def copies(kind, d):
        e = d ^ 1
        if kind == 0:
            if d < 2:
                x = 0 if d == 0 else X - 1
                return [halo(0, d, occ_v.at[x], ix_in.at[e, 0]),
                        halo(1, d, reg_v.at[x], ix_in.at[e, 1])]
            return [halo(0, d, iy_send.at[d - 2, 0], iy_in.at[e - 2, 0]),
                    halo(1, d, iy_send.at[d - 2, 1], iy_in.at[e - 2, 1])]
        if kind == 1:
            return [halo(2, d, c_v, c_in.at[e])]
        p = kind - 2
        if d < 2:
            return [halo(3 + p, d, wx_send.at[p, d], wx_in.at[p, e])]
        return [halo(3 + p, d, wy_send.at[p, d - 2], wy_in.at[p, e - 2])]

    def halo_start(kind):
        for d in range(4):
            @pl.when(has[d])
            def _():
                for c in copies(kind, d):
                    c.start()

    def halo_wait(kind):
        for d in range(4):
            @pl.when(has[d])
            def _():
                for c in copies(kind, d ^ 1):
                    c.wait_recv()

    def halo_done(kind):
        for d in range(4):
            @pl.when(has[d])
            def _():
                for c in copies(kind, d):
                    c.wait_send()

    loads[2].wait()
    acc = lax.fori_loop(0, X, lambda x, a: add_rc(a, reg_v[x], [r_v[c, x] for c in range(3)]),
                        zero_acc(ncr))
    make_row(0, acc, 0)
    loads[3].wait()

    pl.semaphore_wait(barrier, ND - 1)
    halo_start(0)
    gather_start(0)
    halo_start(1)

    def stiff_of(o):
        return soft_stiff + (bone_stiff - soft_stiff) * o.astype(f32)

    def own_k(x, _):
        k_p[x + 1] = stiff_of(occ_v[x])
        return 0

    lax.fori_loop(0, X, own_k, 0)
    halo_wait(0)
    for d in range(2):
        @pl.when(has[d])
        def _():
            k_p[0 if d == 0 else X + 1] = stiff_of(ix_in[d, 0])

        @pl.when(jnp.logical_not(has[d]))
        def _():
            k_p[0 if d == 0 else X + 1] = jnp.zeros((Y, Z), f32)

    row_id = lax.broadcasted_iota(jnp.int32, (Y, Z), 0)
    lane_id = lax.broadcasted_iota(jnp.int32, (Y, Z), 1)
    side_lo = jnp.where(has[2], 1.0, 0.0).astype(f32)
    side_hi = jnp.where(has[3], 1.0, 0.0).astype(f32)

    def yshift(u, lo, hi):
        down = jnp.where(row_id == 0, lo, pltpu.roll(u, 1, 0))
        up = jnp.where(row_id == Y - 1, hi, pltpu.roll(u, Y - 1, 0))
        return down, up

    def save_faces(p, x, w):
        for c in range(3):
            wy_send[p, 0, c, pl.ds(x, 1), :] = w[c][0:1, :]
            wy_send[p, 1, c, pl.ds(x, 1), :] = w[c][Y - 1:Y, :]

    def coefficients(x, _):
        k = k_p[x + 1]
        lo = stiff_of(iy_in[0, 0, pl.ds(x, 1), :]) * side_lo
        hi = stiff_of(iy_in[1, 0, pl.ds(x, 1), :]) * side_hi
        down, up = yshift(k, lo, hi)
        back = jnp.where(lane_id == 0, 0.0, pltpu.roll(k, 1, 1))
        ahead = jnp.where(lane_id == Z - 1, 0.0, pltpu.roll(k, Z - 1, 1))
        xm = 0.5 * (k + k_p[x])
        xp = 0.5 * (k + k_p[x + 2])
        ym = 0.5 * (k + down)
        yp = 0.5 * (k + up)
        zm = 0.5 * (k + back)
        zp = 0.5 * (k + ahead)
        diag = xm + xp + ym + yp + zm + zp + 0.5 * k
        inv = 1.0 / diag
        kx[x] = xm
        kx[x + 1] = xp
        kym[x] = ym
        kyp[x] = yp
        kzm[x] = jnp.where(lane_id == 0, 0.0, zm)
        kzp[x] = jnp.where(lane_id == Z - 1, 0.0, zp)
        dg[x] = diag - 0.25 * k
        invd[x] = inv
        w = [r_v[c, x] * inv for c in range(3)]
        for c in range(3):
            z_p[c, x + 1] = w[c]
        save_faces(0, x, w)
        return 0

    lax.fori_loop(0, X, coefficients, 0)
    for c in range(3):
        wx_send[0, 0, c] = z_p[c, 1]
        wx_send[0, 1, c] = z_p[c, X]
    halo_start(2)

    def edges(p, qs, pad, side):
        for d in range(2):
            s = spread(ix_in[d, 1], qs[d])
            for c in range(3):
                pad[c, 0 if d == 0 else X + 1] = wx_in[p, d, c] + s[c]
        for d in range(2):
            s = spread(iy_in[d, 1], qs[2 + d])
            for c in range(3):
                side[d, c] = wy_in[p, d, c] + s[c]

    def operate(pad, side, x):
        k = k_p[x + 1]
        u = [pad[c, x + 1] for c in range(3)]
        k4 = 0.25 * k * (u[0] + u[1] + u[2])
        out = []
        for c in range(3):
            down, up = yshift(u[c], side[0, c, pl.ds(x, 1), :], side[1, c, pl.ds(x, 1), :])
            a = dg[x] * u[c] + k4
            a = a - (kx[x] * pad[c, x] + kx[x + 1] * pad[c, x + 2])
            a = a - (kym[x] * down + kyp[x] * up)
            a = a - (kzm[x] * pltpu.roll(u[c], 1, 1) + kzp[x] * pltpu.roll(u[c], Z - 1, 1))
            out.append(a)
        return u, out

    gather_wait(0, ag_recv)
    halo_wait(1)
    tiles = coarse_vector(0)
    q = answers(tiles, c_v)
    qs = [answers(tiles, c_in.at[d]) for d in range(4)]

    def add_spread(x, _):
        s = spread(reg_v[x], q)
        for c in range(3):
            z_p[c, x + 1] = z_p[c, x + 1] + s[c]
        return 0

    lax.fori_loop(0, X, add_spread, 0)
    halo_wait(2)
    edges(0, qs, z_p, zy)

    def dots(a, b):
        return fold(a[0] * b[0] + a[1] * b[1] + a[2] * b[2])

    def first(x, carry):
        u, a = operate(z_p, zy, x)
        r = [r_v[c, x] for c in range(3)]
        w = []
        for c in range(3):
            y_v[c, x] = a[c]
            w.append(a[c] * invd[x])
            v_p[c, x + 1] = w[c]
        save_faces(1, x, w)
        acc = add_rc(carry[:ncr], reg_v[x], a)
        return acc + (carry[ncr] + dots(r, u), carry[ncr + 1] + dots(a, u))

    acc = lax.fori_loop(0, X, first, zero_acc(ncr + 2))
    make_row(1, acc, 0)
    gather_start(1)
    for c in range(3):
        wx_send[1, 0, c] = v_p[c, 1]
        wx_send[1, 1, c] = v_p[c, X]
    halo_start(3)
    halo_wait(3)
    gather_wait(1, ag_recv)
    tiles = coarse_vector(1)
    q = answers(tiles, c_v)
    qs = [answers(tiles, c_in.at[d]) for d in range(4)]
    rz0 = total(1, 0)
    alpha0 = rz0 / total(1, 1)

    def add_spread_v(x, _):
        s = spread(reg_v[x], q)
        for c in range(3):
            v_p[c, x + 1] = v_p[c, x + 1] + s[c]
        return 0

    lax.fori_loop(0, X, add_spread_v, 0)
    edges(1, qs, v_p, vy)

    def second(x, carry):
        u, a = operate(v_p, vy, x)
        r, z, az = [], [], []
        for c in range(3):
            y = y_v[c, x]
            r.append(r_v[c, x] - alpha0 * y)
            z.append(z_p[c, x + 1] - alpha0 * u[c])
            az.append(y - alpha0 * a[c])
            r_v[c, x] = r[c]
            x_out[c, x] = z[c]
            az_v[c, x] = az[c]
        return (carry[0] + dots(r, z), carry[1] + dots(az, z))

    acc = lax.fori_loop(0, X, second, zero_acc(2))
    make_row(2, acc, ncr)
    gather_start(2)
    gather_wait(2, ag_recv)
    rz1 = total(2, 0)
    beta = rz1 / rz0
    alpha1 = rz1 / (total(2, 1) - beta * rz1 / alpha0)
    along = alpha0 + alpha1 * beta
    a1b = alpha1 * beta

    def last(x, _):
        for c in range(3):
            x_out[c, x] = along * z_p[c, x + 1] + alpha1 * x_out[c, x]
            res_out[c, x] = r_v[c, x] - alpha1 * az_v[c, x] - a1b * y_v[c, x]
        return 0

    lax.fori_loop(0, X, last, 0)
    for kind in range(4):
        halo_done(kind)
    for p in range(3):
        gather_wait(p, ag_send)


def local(nw, nn, right_side, occupancy, region, coarse_inverse):
    _, X, Y, Z = right_side.shape
    ncr, NC = coarse_inverse.shape
    ND = nw * nn
    f32, i32 = jnp.float32, jnp.int32
    V = pltpu.VMEM
    field, pad, scal = (3, X, Y, Z), (3, X + 2, Y, Z), (X, Y, Z)
    scratch = [
        V(field, f32), V(scal, i32), V(scal, i32), V((ncr, NC), f32),
        V((X + 2, Y, Z), f32), V((X + 1, Y, Z), f32),
        V(scal, f32), V(scal, f32), V(scal, f32), V(scal, f32), V(scal, f32), V(scal, f32),
        V(pad, f32), V(field, f32), V(pad, f32), V(field, f32),
        V((2, 3, X, Z), f32), V((2, 3, X, Z), f32),
        V((2, 2, Y, Z), i32), V((2, 2, X, Z), i32), V((2, 2, X, Z), i32),
        V((4, ncr, NC), f32),
        V((2, 2, 3, Y, Z), f32), V((2, 2, 3, Y, Z), f32),
        V((2, 2, 3, X, Z), f32), V((2, 2, 3, X, Z), f32),
        V((3, SUB, LANES), f32), V((3, ND, LANES), f32),
        pltpu.SemaphoreType.DMA((4,)),
        pltpu.SemaphoreType.DMA((5, 4)), pltpu.SemaphoreType.DMA((5, 4)),
        pltpu.SemaphoreType.DMA((3,)), pltpu.SemaphoreType.DMA((3,)),
    ]
    return pl.pallas_call(
        functools.partial(kernel, nw, nn),
        out_shape=(jax.ShapeDtypeStruct(field, f32), jax.ShapeDtypeStruct(field, f32)),
        in_specs=[pl.BlockSpec(memory_space=pl.ANY)] * 4,
        out_specs=(pl.BlockSpec(memory_space=pltpu.VMEM),) * 2,
        scratch_shapes=scratch,
        compiler_params=pltpu.CompilerParams(collective_id=0, has_side_effects=True),
    )(right_side, occupancy, region, coarse_inverse)


def solution(mesh):
    return jax.shard_map(
        functools.partial(local, mesh.shape["wide"], mesh.shape["narrow"]),
        mesh=mesh,
        in_specs=(
            P(None, "wide", "narrow", None),
            P("wide", "narrow", None),
            P("wide", "narrow", None),
            P(("wide", "narrow"), None),
        ),
        out_specs=(P(None, "wide", "narrow", None), P(None, "wide", "narrow", None)),
        check_vma=False,
    )
```

```python
import functools

import jax
import jax.numpy as jnp
from jax import lax
from jax.experimental import pallas as pl
from jax.experimental.pallas import tpu as pltpu
from jax.sharding import PartitionSpec as P

LANES = 128
SUB = 8
UNROLL = 16
looped = functools.partial(lax.fori_loop, unroll=UNROLL)
MESH = pl.DeviceIdType.MESH
bone_stiff = 1.0
soft_stiff = 0.1


def kernel(nw, nn, r_hbm, occ_hbm, reg_hbm, ci_hbm,
           z0_v, z1_v, r_v, az_v, y_v, sc_v,
            occ_v, reg_v, c_v, k_p, kx, kym, kyp, kzm, kzp, dg, invd,
           z_p, v_p, zy, vy,
           ix_in, iy_send, iy_in, c_in, wx_send, wx_in, wy_send, wy_in,
           row_send, rows, load_sem, hs_send, hs_recv, ag_send, ag_recv):
    X, Y, Z = occ_v.shape
    ncr, NC = c_v.shape
    G = ncr // 3
    ND = nw * nn
    wi = lax.axis_index("wide")
    ni = lax.axis_index("narrow")
    me = wi * nn + ni
    f32 = jnp.float32

    loads = [pltpu.make_async_copy(s, d, load_sem.at[i]) for i, (s, d) in enumerate(
        ((occ_hbm, occ_v), (reg_hbm, reg_v), (r_hbm, r_v), (ci_hbm, c_v)))]
    for l in loads:
        l.start()

    def peer(i):
        t = lax.rem(me + i, ND)
        return (t // nn, lax.rem(t, nn))

    barrier = pltpu.get_barrier_semaphore()

    def greet(i, _):
        pl.semaphore_signal(barrier, inc=1, device_id=peer(i), device_id_type=MESH)
        return 0

    lax.fori_loop(1, ND, greet, 0, unroll=ND <= 64)

    has = (wi > 0, wi < nw - 1, ni > 0, ni < nn - 1)
    to = ((wi - 1, ni), (wi + 1, ni), (wi, ni - 1), (wi, ni + 1))

    for d in range(4):
        @pl.when(jnp.logical_not(has[d]))
        def _():
            c_in[d] = jnp.zeros((ncr, NC), f32)
            for p in range(2):
                if d < 2:
                    wx_in[p, d] = jnp.zeros((3, Y, Z), f32)
                else:
                    wy_in[p, d - 2] = jnp.zeros((3, X, Z), f32)
            if d < 2:
                ix_in[d] = jnp.zeros((2, Y, Z), jnp.int32)
            else:
                iy_in[d - 2] = jnp.zeros((2, X, Z), jnp.int32)

    loads[0].wait()
    loads[1].wait()

    def pack_ints(x, _):
        iy_send[0, 0, pl.ds(x, 1), :] = occ_v[x, 0:1, :]
        iy_send[1, 0, pl.ds(x, 1), :] = occ_v[x, Y - 1:Y, :]
        iy_send[0, 1, pl.ds(x, 1), :] = reg_v[x, 0:1, :]
        iy_send[1, 1, pl.ds(x, 1), :] = reg_v[x, Y - 1:Y, :]
        return 0

    looped(0, X, pack_ints, 0)

    def fold(a):
        return jnp.sum(a.reshape(Y // SUB, SUB, Z), axis=0)

    def zero_acc(n):
        return tuple(jnp.zeros((SUB, Z), f32) for _ in range(n))

    def add_rc(acc, reg, u):
        out = list(acc)
        for g in range(G):
            m = reg == g
            for c in range(3):
                out[g * 3 + c] = acc[g * 3 + c] + fold(jnp.where(m, u[c], 0.0))
        return tuple(out)

    base = (me * ncr) % LANES

    def make_row(p, acc, first):
        a = jnp.concatenate([jnp.sum(b, axis=0, keepdims=True) for b in acc], axis=0)
        col = jnp.sum(a, axis=1, keepdims=True)
        n = len(acc)
        k = lax.broadcasted_iota(jnp.int32, (n, LANES), 0)
        lane = lax.broadcasted_iota(jnp.int32, (n, LANES), 1)
        target = (base + first + k) & (LANES - 1)
        row = jnp.sum(jnp.where(lane == target, col, 0.0), axis=0, keepdims=True)
        row_send[p, 0:1, :] = row
        rows[p, pl.ds(me, 1), :] = row

    def gather_start(p):
        def send(i, _):
            pltpu.make_async_remote_copy(
                src_ref=row_send.at[p, pl.ds(0, 1)], dst_ref=rows.at[p, pl.ds(me, 1)],
                send_sem=ag_send.at[p], recv_sem=ag_recv.at[p],
                device_id=peer(i), device_id_type=MESH).start()
            return 0
        lax.fori_loop(1, ND, send, 0, unroll=ND <= 64)

    def gather_wait(p, sem):
        part = rows.at[p, pl.ds(0, ND - 1)]
        pltpu.make_async_copy(part, part, sem.at[p]).wait()

    def coarse_vector(p):
        tiles = []
        for t in range(NC // LANES):
            lo = (LANES * t) // ncr // SUB * SUB
            hi = min(ND, -(-(-(-(LANES * (t + 1)) // ncr)) // SUB) * SUB)
            d = lax.broadcasted_iota(jnp.int32, (hi - lo, LANES), 0) + lo
            j = lax.broadcasted_iota(jnp.int32, (hi - lo, LANES), 1) + LANES * t
            m = (j >= d * ncr) & (j < d * ncr + ncr)
            tiles.append(jnp.sum(jnp.where(m, rows[p, lo:hi, :], 0.0), axis=0, keepdims=True))
        return tiles

    def total(p, s):
        d = lax.broadcasted_iota(jnp.int32, (ND, LANES), 0)
        lane = lax.broadcasted_iota(jnp.int32, (ND, LANES), 1)
        m = lane == ((d * ncr + ncr + s) & (LANES - 1))
        v = jnp.sum(jnp.where(m, rows[p], 0.0), axis=0, keepdims=True)
        return jnp.sum(v, axis=1, keepdims=True)

    def answers(tiles, ref):
        s = ref[:, 0:LANES] * tiles[0]
        for t in range(1, len(tiles)):
            s = s + ref[:, t * LANES:(t + 1) * LANES] * tiles[t]
        q = jnp.sum(s, axis=1, keepdims=True)
        return [q[i:i + 1, :] for i in range(ncr)]

    def spread(reg, q):
        masks = [reg == g for g in range(G)]
        out = []
        for c in range(3):
            s = jnp.zeros(reg.shape, f32)
            for g in range(G):
                s = jnp.where(masks[g], q[g * 3 + c], s)
            out.append(s)
        return out

    def halo(slot, d, src, dst):
        return pltpu.make_async_remote_copy(
            src_ref=src, dst_ref=dst, send_sem=hs_send.at[slot, d],
            recv_sem=hs_recv.at[slot, d ^ 1], device_id=to[d], device_id_type=MESH)

    def copies(kind, d):
        e = d ^ 1
        if kind == 0:
            if d < 2:
                x = 0 if d == 0 else X - 1
                return [halo(0, d, occ_v.at[x], ix_in.at[e, 0]),
                        halo(1, d, reg_v.at[x], ix_in.at[e, 1])]
            return [halo(0, d, iy_send.at[d - 2, 0], iy_in.at[e - 2, 0]),
                    halo(1, d, iy_send.at[d - 2, 1], iy_in.at[e - 2, 1])]
        if kind == 1:
            return [halo(2, d, c_v, c_in.at[e])]
        p = kind - 2
        if d < 2:
            return [halo(3 + p, d, wx_send.at[p, d], wx_in.at[p, e])]
        return [halo(3 + p, d, wy_send.at[p, d - 2], wy_in.at[p, e - 2])]

    def halo_start(kind):
        for d in range(4):
            @pl.when(has[d])
            def _():
                for c in copies(kind, d):
                    c.start()

    def halo_wait(kind):
        for d in range(4):
            @pl.when(has[d])
            def _():
                for c in copies(kind, d ^ 1):
                    c.wait_recv()

    def halo_done(kind):
        for d in range(4):
            @pl.when(has[d])
            def _():
                for c in copies(kind, d):
                    c.wait_send()

    loads[2].wait()
    acc = looped(0, X, lambda x, a: add_rc(a, reg_v[x], [r_v[c, x] for c in range(3)]),
                        zero_acc(ncr))
    make_row(0, acc, 0)
    loads[3].wait()

    pl.semaphore_wait(barrier, ND - 1)
    halo_start(0)
    gather_start(0)
    halo_start(1)

    def stiff_of(o):
        return soft_stiff + (bone_stiff - soft_stiff) * o.astype(f32)

    def own_k(x, _):
        k_p[x + 1] = stiff_of(occ_v[x])
        return 0

    looped(0, X, own_k, 0)
    halo_wait(0)
    for d in range(2):
        @pl.when(has[d])
        def _():
            k_p[0 if d == 0 else X + 1] = stiff_of(ix_in[d, 0])

        @pl.when(jnp.logical_not(has[d]))
        def _():
            k_p[0 if d == 0 else X + 1] = jnp.zeros((Y, Z), f32)

    row_id = lax.broadcasted_iota(jnp.int32, (Y, Z), 0)
    lane_id = lax.broadcasted_iota(jnp.int32, (Y, Z), 1)
    side_lo = jnp.where(has[2], 1.0, 0.0).astype(f32)
    side_hi = jnp.where(has[3], 1.0, 0.0).astype(f32)

    def yshift(u, lo, hi):
        down = jnp.where(row_id == 0, lo, pltpu.roll(u, 1, 0))
        up = jnp.where(row_id == Y - 1, hi, pltpu.roll(u, Y - 1, 0))
        return down, up

    def save_faces(p, x, w):
        for c in range(3):
            wy_send[p, 0, c, pl.ds(x, 1), :] = w[c][0:1, :]
            wy_send[p, 1, c, pl.ds(x, 1), :] = w[c][Y - 1:Y, :]

    def coefficients(x, _):
        k = k_p[x + 1]
        lo = stiff_of(iy_in[0, 0, pl.ds(x, 1), :]) * side_lo
        hi = stiff_of(iy_in[1, 0, pl.ds(x, 1), :]) * side_hi
        down, up = yshift(k, lo, hi)
        back = jnp.where(lane_id == 0, 0.0, pltpu.roll(k, 1, 1))
        ahead = jnp.where(lane_id == Z - 1, 0.0, pltpu.roll(k, Z - 1, 1))
        xm = 0.5 * (k + k_p[x])
        xp = 0.5 * (k + k_p[x + 2])
        ym = 0.5 * (k + down)
        yp = 0.5 * (k + up)
        zm = 0.5 * (k + back)
        zp = 0.5 * (k + ahead)
        diag = xm + xp + ym + yp + zm + zp + 0.5 * k
        inv = 1.0 / diag
        kx[x] = xm
        kx[x + 1] = xp
        kym[x] = ym
        kyp[x] = yp
        kzm[x] = jnp.where(lane_id == 0, 0.0, zm)
        kzp[x] = jnp.where(lane_id == Z - 1, 0.0, zp)
        dg[x] = diag - 0.25 * k
        invd[x] = inv
        w = [r_v[c, x] * inv for c in range(3)]
        for c in range(3):
            z_p[c, x + 1] = w[c]
        save_faces(0, x, w)
        return 0

    looped(0, X, coefficients, 0)
    for c in range(3):
        wx_send[0, 0, c] = z_p[c, 1]
        wx_send[0, 1, c] = z_p[c, X]
    halo_start(2)

    def edges(p, qs, pad, side):
        for d in range(2):
            s = spread(ix_in[d, 1], qs[d])
            for c in range(3):
                pad[c, 0 if d == 0 else X + 1] = wx_in[p, d, c] + s[c]
        for d in range(2):
            s = spread(iy_in[d, 1], qs[2 + d])
            for c in range(3):
                side[d, c] = wy_in[p, d, c] + s[c]

    def operate(pad, side, x):
        k = k_p[x + 1]
        u = [pad[c, x + 1] for c in range(3)]
        k4 = 0.25 * k * (u[0] + u[1] + u[2])
        out = []
        for c in range(3):
            down, up = yshift(u[c], side[0, c, pl.ds(x, 1), :], side[1, c, pl.ds(x, 1), :])
            a = dg[x] * u[c] + k4
            a = a - (kx[x] * pad[c, x] + kx[x + 1] * pad[c, x + 2])
            a = a - (kym[x] * down + kyp[x] * up)
            a = a - (kzm[x] * pltpu.roll(u[c], 1, 1) + kzp[x] * pltpu.roll(u[c], Z - 1, 1))
            out.append(a)
        return u, out

    gather_wait(0, ag_recv)
    halo_wait(1)
    tiles = coarse_vector(0)
    q = answers(tiles, c_v)
    qs = [answers(tiles, c_in.at[d]) for d in range(4)]

    def add_spread(x, _):
        s = spread(reg_v[x], q)
        for c in range(3):
            z = z_p[c, x + 1] + s[c]
            z_p[c, x + 1] = z
            z0_v[c, x] = z
        return 0

    looped(0, X, add_spread, 0)
    halo_wait(2)
    edges(0, qs, z_p, zy)

    def dots(a, b):
        return fold(a[0] * b[0] + a[1] * b[1] + a[2] * b[2])

    def first(x, carry):
        u, a = operate(z_p, zy, x)
        r = [r_v[c, x] for c in range(3)]
        w = []
        for c in range(3):
            y_v[c, x] = a[c]
            w.append(a[c] * invd[x])
            v_p[c, x + 1] = w[c]
        save_faces(1, x, w)
        acc = add_rc(carry[:ncr], reg_v[x], a)
        return acc + (carry[ncr] + dots(r, u), carry[ncr + 1] + dots(a, u))

    acc = looped(0, X, first, zero_acc(ncr + 2))
    make_row(1, acc, 0)
    gather_start(1)
    for c in range(3):
        wx_send[1, 0, c] = v_p[c, 1]
        wx_send[1, 1, c] = v_p[c, X]
    halo_start(3)
    halo_wait(3)
    gather_wait(1, ag_recv)
    tiles = coarse_vector(1)
    q = answers(tiles, c_v)
    qs = [answers(tiles, c_in.at[d]) for d in range(4)]
    rz0 = total(1, 0)
    alpha0 = rz0 / total(1, 1)

    def add_spread_v(x, _):
        s = spread(reg_v[x], q)
        for c in range(3):
            v_p[c, x + 1] = v_p[c, x + 1] + s[c]
        return 0

    looped(0, X, add_spread_v, 0)
    edges(1, qs, v_p, vy)

    def second(x, carry):
        u, a = operate(v_p, vy, x)
        r, z, az = [], [], []
        for c in range(3):
            y = y_v[c, x]
            r.append(r_v[c, x] - alpha0 * y)
            z.append(z_p[c, x + 1] - alpha0 * u[c])
            az.append(y - alpha0 * a[c])
            r_v[c, x] = r[c]
            z1_v[c, x] = z[c]
            az_v[c, x] = az[c]
        return (carry[0] + dots(r, z), carry[1] + dots(az, z))

    acc = looped(0, X, second, zero_acc(2))
    make_row(2, acc, ncr)
    gather_start(2)
    gather_wait(2, ag_recv)
    rz1 = total(2, 0)
    beta = rz1 / rz0
    alpha1 = rz1 / (total(2, 1) - beta * rz1 / alpha0)
    along = alpha0 + alpha1 * beta
    a1b = alpha1 * beta

    sc_v[0:1, :] = jnp.broadcast_to(along, (1, LANES))
    sc_v[1:2, :] = jnp.broadcast_to(alpha1, (1, LANES))
    sc_v[2:3, :] = jnp.broadcast_to(a1b, (1, LANES))
    for kind in range(4):
        halo_done(kind)
    for p in range(3):
        gather_wait(p, ag_send)


def finish(z0_v, z1_v, r_v, az_v, y_v, sc_v, x_out, res_out):
    c = pl.program_id(0)
    along = sc_v[0:1, 0:1]
    alpha1 = sc_v[1:2, 0:1]
    a1b = sc_v[2:3, 0:1]
    for x in range(x_out.shape[1]):
        x_out[0, x] = along * z0_v[c, x] + alpha1 * z1_v[c, x]
        res_out[0, x] = r_v[c, x] - alpha1 * az_v[c, x] - a1b * y_v[c, x]


def local(nw, nn, right_side, occupancy, region, coarse_inverse):
    _, X, Y, Z = right_side.shape
    ncr, NC = coarse_inverse.shape
    ND = nw * nn
    f32, i32 = jnp.float32, jnp.int32
    V = pltpu.VMEM
    field, pad, scal = (3, X, Y, Z), (3, X + 2, Y, Z), (X, Y, Z)
    scratch = [
        V(scal, i32), V(scal, i32), V((ncr, NC), f32),
        V((X + 2, Y, Z), f32), V((X + 1, Y, Z), f32),
        V(scal, f32), V(scal, f32), V(scal, f32), V(scal, f32), V(scal, f32), V(scal, f32),
        V(pad, f32), V(pad, f32),
        V((2, 3, X, Z), f32), V((2, 3, X, Z), f32),
        V((2, 2, Y, Z), i32), V((2, 2, X, Z), i32), V((2, 2, X, Z), i32),
        V((4, ncr, NC), f32),
        V((2, 2, 3, Y, Z), f32), V((2, 2, 3, Y, Z), f32),
        V((2, 2, 3, X, Z), f32), V((2, 2, 3, X, Z), f32),
        V((3, SUB, LANES), f32), V((3, ND, LANES), f32),
        pltpu.SemaphoreType.DMA((4,)),
        pltpu.SemaphoreType.DMA((5, 4)), pltpu.SemaphoreType.DMA((5, 4)),
        pltpu.SemaphoreType.DMA((3,)), pltpu.SemaphoreType.DMA((3,)),
    ]
    parts = pl.pallas_call(
        functools.partial(kernel, nw, nn),
        out_shape=(V(field, f32),) * 5 + (V((SUB, LANES), f32),),
        in_specs=[pl.BlockSpec(memory_space=pltpu.HBM)] * 4,
        out_specs=(pl.BlockSpec(memory_space=pltpu.VMEM),) * 6,
        scratch_shapes=scratch,
        compiler_params=pltpu.CompilerParams(collective_id=0, has_side_effects=True, vmem_limit_bytes=32 * 1024 * 1024),
    )(*[pltpu.with_memory_space_constraint(a, pltpu.HBM) for a in (right_side, occupancy, region, coarse_inverse)])
    block = pl.BlockSpec((1, X, Y, Z), lambda c: (c, 0, 0, 0))
    return pl.pallas_call(
        finish,
        grid=(3,),
        out_shape=(jax.ShapeDtypeStruct(field, f32),) * 2,
        in_specs=[pl.BlockSpec(memory_space=pltpu.VMEM)] * 6,
        out_specs=(block, block),
        compiler_params=pltpu.CompilerParams(vmem_limit_bytes=16 * 1024 * 1024),
    )(*parts)


def solution(mesh):
    return jax.shard_map(
        functools.partial(local, mesh.shape["wide"], mesh.shape["narrow"]),
        mesh=mesh,
        in_specs=(
            P(None, "wide", "narrow", None),
            P("wide", "narrow", None),
            P("wide", "narrow", None),
            P(("wide", "narrow"), None),
        ),
        out_specs=(P(None, "wide", "narrow", None), P(None, "wide", "narrow", None)),
        check_vma=False,
    )
```

```python
import functools

import jax
import jax.numpy as jnp
from jax import lax
from jax.experimental import pallas as pl
from jax.experimental.pallas import tpu as pltpu
from jax.sharding import PartitionSpec as P

LANES = 128
SUB = 8
UNROLL = 16
looped = functools.partial(lax.fori_loop, unroll=UNROLL)
MESH = pl.DeviceIdType.MESH
bone_stiff = 1.0
soft_stiff = 0.1


def kernel(nw, nn, r_hbm, occ_hbm, reg_hbm, ci_hbm,
           z0_v, z1_v, r_v, az_v, y_v, sc_v,
            occ_v, reg_v, c_v, k_p, kx, kym, kyp, kzm, kzp, dg, invd,
           z_p, v_p, zy, vy,
           ix_in, iy_send, iy_in, c_in, wx_send, wx_in, wy_send, wy_in,
           row_send, rows, load_sem, hs_send, hs_recv, ag_send, ag_recv):
    X, Y, Z = occ_v.shape
    ncr, NC = c_v.shape
    G = ncr // 3
    ND = nw * nn
    wi = lax.axis_index("wide")
    ni = lax.axis_index("narrow")
    me = wi * nn + ni
    f32 = jnp.float32

    loads = [pltpu.make_async_copy(s, d, load_sem.at[i]) for i, (s, d) in enumerate(
        ((occ_hbm, occ_v), (reg_hbm, reg_v), (r_hbm, r_v), (ci_hbm, c_v)))]
    for l in loads:
        l.start()

    def peer(i):
        t = lax.rem(me + i, ND)
        return (t // nn, lax.rem(t, nn))

    barrier = pltpu.get_barrier_semaphore()

    def greet(i, _):
        pl.semaphore_signal(barrier, inc=1, device_id=peer(i), device_id_type=MESH)
        return 0

    lax.fori_loop(1, ND, greet, 0, unroll=ND <= 64)

    has = (wi > 0, wi < nw - 1, ni > 0, ni < nn - 1)
    to = ((wi - 1, ni), (wi + 1, ni), (wi, ni - 1), (wi, ni + 1))

    for d in range(4):
        @pl.when(jnp.logical_not(has[d]))
        def _():
            c_in[d] = jnp.zeros((ncr, NC), f32)
            for p in range(2):
                if d < 2:
                    wx_in[p, d] = jnp.zeros((3, Y, Z), f32)
                else:
                    wy_in[p, d - 2] = jnp.zeros((3, X, Z), f32)
            if d < 2:
                ix_in[d] = jnp.zeros((2, Y, Z), jnp.int32)
            else:
                iy_in[d - 2] = jnp.zeros((2, X, Z), jnp.int32)

    loads[0].wait()
    loads[1].wait()

    def pack_ints(x, _):
        iy_send[0, 0, pl.ds(x, 1), :] = occ_v[x, 0:1, :]
        iy_send[1, 0, pl.ds(x, 1), :] = occ_v[x, Y - 1:Y, :]
        iy_send[0, 1, pl.ds(x, 1), :] = reg_v[x, 0:1, :]
        iy_send[1, 1, pl.ds(x, 1), :] = reg_v[x, Y - 1:Y, :]
        return 0

    looped(0, X, pack_ints, 0)

    def fold(a):
        return jnp.sum(a.reshape(Y // SUB, SUB, Z), axis=0)

    def zero_acc(n):
        return tuple(jnp.zeros((SUB, Z), f32) for _ in range(n))

    def add_rc(acc, reg, u):
        out = list(acc)
        for g in range(G):
            m = reg == g
            for c in range(3):
                out[g * 3 + c] = acc[g * 3 + c] + fold(jnp.where(m, u[c], 0.0))
        return tuple(out)

    base = (me * ncr) % LANES

    def make_row(p, acc, first):
        a = jnp.concatenate([jnp.sum(b, axis=0, keepdims=True) for b in acc], axis=0)
        col = jnp.sum(a, axis=1, keepdims=True)
        n = len(acc)
        k = lax.broadcasted_iota(jnp.int32, (n, LANES), 0)
        lane = lax.broadcasted_iota(jnp.int32, (n, LANES), 1)
        target = (base + first + k) & (LANES - 1)
        row = jnp.sum(jnp.where(lane == target, col, 0.0), axis=0, keepdims=True)
        row_send[p, 0:1, :] = row
        rows[p, pl.ds(me, 1), :] = row

    def gather_start(p):
        def send(i, _):
            pltpu.make_async_remote_copy(
                src_ref=row_send.at[p, pl.ds(0, 1)], dst_ref=rows.at[p, pl.ds(me, 1)],
                send_sem=ag_send.at[p], recv_sem=ag_recv.at[p],
                device_id=peer(i), device_id_type=MESH).start()
            return 0
        lax.fori_loop(1, ND, send, 0, unroll=ND <= 64)

    def gather_wait(p, sem):
        part = rows.at[p, pl.ds(0, ND - 1)]
        pltpu.make_async_copy(part, part, sem.at[p]).wait()

    def coarse_vector(p):
        tiles = []
        for t in range(NC // LANES):
            lo = (LANES * t) // ncr // SUB * SUB
            hi = min(ND, -(-(-(-(LANES * (t + 1)) // ncr)) // SUB) * SUB)
            d = lax.broadcasted_iota(jnp.int32, (hi - lo, LANES), 0) + lo
            j = lax.broadcasted_iota(jnp.int32, (hi - lo, LANES), 1) + LANES * t
            m = (j >= d * ncr) & (j < d * ncr + ncr)
            tiles.append(jnp.sum(jnp.where(m, rows[p, lo:hi, :], 0.0), axis=0, keepdims=True))
        return tiles

    def total(p, s):
        d = lax.broadcasted_iota(jnp.int32, (ND, LANES), 0)
        lane = lax.broadcasted_iota(jnp.int32, (ND, LANES), 1)
        m = lane == ((d * ncr + ncr + s) & (LANES - 1))
        v = jnp.sum(jnp.where(m, rows[p], 0.0), axis=0, keepdims=True)
        return jnp.sum(v, axis=1, keepdims=True)

    def answers(tiles, ref):
        s = ref[:, 0:LANES] * tiles[0]
        for t in range(1, len(tiles)):
            s = s + ref[:, t * LANES:(t + 1) * LANES] * tiles[t]
        q = jnp.sum(s, axis=1, keepdims=True)
        return [q[i:i + 1, :] for i in range(ncr)]

    def spread(reg, q):
        masks = [reg == g for g in range(G)]
        out = []
        for c in range(3):
            s = jnp.zeros(reg.shape, f32)
            for g in range(G):
                s = jnp.where(masks[g], q[g * 3 + c], s)
            out.append(s)
        return out

    def halo(slot, d, src, dst):
        return pltpu.make_async_remote_copy(
            src_ref=src, dst_ref=dst, send_sem=hs_send.at[slot, d],
            recv_sem=hs_recv.at[slot, d ^ 1], device_id=to[d], device_id_type=MESH)

    def copies(kind, d):
        e = d ^ 1
        if kind == 0:
            if d < 2:
                x = 0 if d == 0 else X - 1
                return [halo(0, d, occ_v.at[x], ix_in.at[e, 0]),
                        halo(1, d, reg_v.at[x], ix_in.at[e, 1])]
            return [halo(0, d, iy_send.at[d - 2, 0], iy_in.at[e - 2, 0]),
                    halo(1, d, iy_send.at[d - 2, 1], iy_in.at[e - 2, 1])]
        if kind == 1:
            return [halo(2, d, c_v, c_in.at[e])]
        p = kind - 2
        if d < 2:
            return [halo(3 + p, d, wx_send.at[p, d], wx_in.at[p, e])]
        return [halo(3 + p, d, wy_send.at[p, d - 2], wy_in.at[p, e - 2])]

    def halo_start(kind):
        for d in range(4):
            @pl.when(has[d])
            def _():
                for c in copies(kind, d):
                    c.start()

    def halo_wait(kind):
        for d in range(4):
            @pl.when(has[d])
            def _():
                for c in copies(kind, d ^ 1):
                    c.wait_recv()

    def halo_done(kind):
        for d in range(4):
            @pl.when(has[d])
            def _():
                for c in copies(kind, d):
                    c.wait_send()

    loads[2].wait()
    acc = looped(0, X, lambda x, a: add_rc(a, reg_v[x], [r_v[c, x] for c in range(3)]),
                        zero_acc(ncr))
    make_row(0, acc, 0)
    loads[3].wait()

    pl.semaphore_wait(barrier, ND - 1)
    halo_start(0)
    gather_start(0)
    halo_start(1)

    def stiff_of(o):
        return soft_stiff + (bone_stiff - soft_stiff) * o.astype(f32)

    def own_k(x, _):
        k_p[x + 1] = stiff_of(occ_v[x])
        return 0

    looped(0, X, own_k, 0)
    halo_wait(0)
    for d in range(2):
        @pl.when(has[d])
        def _():
            k_p[0 if d == 0 else X + 1] = stiff_of(ix_in[d, 0])

        @pl.when(jnp.logical_not(has[d]))
        def _():
            k_p[0 if d == 0 else X + 1] = jnp.zeros((Y, Z), f32)

    row_id = lax.broadcasted_iota(jnp.int32, (Y, Z), 0)
    lane_id = lax.broadcasted_iota(jnp.int32, (Y, Z), 1)
    side_lo = jnp.where(has[2], 1.0, 0.0).astype(f32)
    side_hi = jnp.where(has[3], 1.0, 0.0).astype(f32)

    def yshift(u, lo, hi):
        down = jnp.where(row_id == 0, lo, pltpu.roll(u, 1, 0))
        up = jnp.where(row_id == Y - 1, hi, pltpu.roll(u, Y - 1, 0))
        return down, up

    def save_faces(p, x, w):
        for c in range(3):
            wy_send[p, 0, c, pl.ds(x, 1), :] = w[c][0:1, :]
            wy_send[p, 1, c, pl.ds(x, 1), :] = w[c][Y - 1:Y, :]

    def coefficients(x, _):
        k = k_p[x + 1]
        lo = stiff_of(iy_in[0, 0, pl.ds(x, 1), :]) * side_lo
        hi = stiff_of(iy_in[1, 0, pl.ds(x, 1), :]) * side_hi
        down, up = yshift(k, lo, hi)
        back = jnp.where(lane_id == 0, 0.0, pltpu.roll(k, 1, 1))
        ahead = jnp.where(lane_id == Z - 1, 0.0, pltpu.roll(k, Z - 1, 1))
        xm = 0.5 * (k + k_p[x])
        xp = 0.5 * (k + k_p[x + 2])
        ym = 0.5 * (k + down)
        yp = 0.5 * (k + up)
        zm = 0.5 * (k + back)
        zp = 0.5 * (k + ahead)
        diag = xm + xp + ym + yp + zm + zp + 0.5 * k
        inv = 1.0 / diag
        kx[x] = xm
        kx[x + 1] = xp
        kym[x] = ym
        kyp[x] = yp
        kzm[x] = jnp.where(lane_id == 0, 0.0, zm)
        kzp[x] = jnp.where(lane_id == Z - 1, 0.0, zp)
        dg[x] = diag - 0.25 * k
        invd[x] = inv
        w = [r_v[c, x] * inv for c in range(3)]
        for c in range(3):
            z_p[c, x + 1] = w[c]
        save_faces(0, x, w)
        return 0

    looped(0, X, coefficients, 0)
    for c in range(3):
        wx_send[0, 0, c] = z_p[c, 1]
        wx_send[0, 1, c] = z_p[c, X]
    halo_start(2)

    def edges(p, qs, pad, side):
        for d in range(2):
            s = spread(ix_in[d, 1], qs[d])
            for c in range(3):
                pad[c, 0 if d == 0 else X + 1] = wx_in[p, d, c] + s[c]
        for d in range(2):
            s = spread(iy_in[d, 1], qs[2 + d])
            for c in range(3):
                side[d, c] = wy_in[p, d, c] + s[c]

    def operate(pad, side, x):
        k = k_p[x + 1]
        u = [pad[c, x + 1] for c in range(3)]
        k4 = 0.25 * k * (u[0] + u[1] + u[2])
        out = []
        for c in range(3):
            down, up = yshift(u[c], side[0, c, pl.ds(x, 1), :], side[1, c, pl.ds(x, 1), :])
            a = dg[x] * u[c] + k4
            a = a - (kx[x] * pad[c, x] + kx[x + 1] * pad[c, x + 2])
            a = a - (kym[x] * down + kyp[x] * up)
            a = a - (kzm[x] * pltpu.roll(u[c], 1, 1) + kzp[x] * pltpu.roll(u[c], Z - 1, 1))
            out.append(a)
        return u, out

    gather_wait(0, ag_recv)
    halo_wait(1)
    tiles = coarse_vector(0)
    q = answers(tiles, c_v)
    qs = [answers(tiles, c_in.at[d]) for d in range(4)]

    def add_spread(x, _):
        s = spread(reg_v[x], q)
        for c in range(3):
            z = z_p[c, x + 1] + s[c]
            z_p[c, x + 1] = z
            z0_v[c, x] = z
        return 0

    looped(0, X, add_spread, 0)
    halo_wait(2)
    edges(0, qs, z_p, zy)

    def dots(a, b):
        return fold(a[0] * b[0] + a[1] * b[1] + a[2] * b[2])

    def first(x, carry):
        u, a = operate(z_p, zy, x)
        r = [r_v[c, x] for c in range(3)]
        w = []
        for c in range(3):
            y_v[c, x] = a[c]
            w.append(a[c] * invd[x])
            v_p[c, x + 1] = w[c]
        save_faces(1, x, w)
        acc = add_rc(carry[:ncr], reg_v[x], a)
        return acc + (carry[ncr] + dots(r, u), carry[ncr + 1] + dots(a, u))

    acc = looped(0, X, first, zero_acc(ncr + 2))
    make_row(1, acc, 0)
    gather_start(1)
    for c in range(3):
        wx_send[1, 0, c] = v_p[c, 1]
        wx_send[1, 1, c] = v_p[c, X]
    halo_start(3)
    halo_wait(3)
    gather_wait(1, ag_recv)
    tiles = coarse_vector(1)
    q = answers(tiles, c_v)
    qs = [answers(tiles, c_in.at[d]) for d in range(4)]
    rz0 = total(1, 0)
    alpha0 = rz0 / total(1, 1)

    def add_spread_v(x, _):
        s = spread(reg_v[x], q)
        for c in range(3):
            v_p[c, x + 1] = v_p[c, x + 1] + s[c]
        return 0

    looped(0, X, add_spread_v, 0)
    edges(1, qs, v_p, vy)

    def second(x, carry):
        u, a = operate(v_p, vy, x)
        r, z, az = [], [], []
        for c in range(3):
            y = y_v[c, x]
            r.append(r_v[c, x] - alpha0 * y)
            z.append(z_p[c, x + 1] - alpha0 * u[c])
            az.append(y - alpha0 * a[c])
            r_v[c, x] = r[c]
            z1_v[c, x] = z[c]
            az_v[c, x] = az[c]
        return (carry[0] + dots(r, z), carry[1] + dots(az, z))

    acc = looped(0, X, second, zero_acc(2))
    make_row(2, acc, ncr)
    gather_start(2)
    gather_wait(2, ag_recv)
    rz1 = total(2, 0)
    beta = rz1 / rz0
    alpha1 = rz1 / (total(2, 1) - beta * rz1 / alpha0)
    along = alpha0 + alpha1 * beta
    a1b = alpha1 * beta

    sc_v[0:1, :] = jnp.broadcast_to(along, (1, LANES))
    sc_v[1:2, :] = jnp.broadcast_to(alpha1, (1, LANES))
    sc_v[2:3, :] = jnp.broadcast_to(a1b, (1, LANES))
    for kind in range(4):
        halo_done(kind)
    for p in range(3):
        gather_wait(p, ag_send)


def finish(z0_v, z1_v, r_v, az_v, y_v, sc_v, x_out, res_out, xb, rb, sem):
    along = sc_v[0:1, 0:1]
    alpha1 = sc_v[1:2, 0:1]
    a1b = sc_v[2:3, 0:1]
    X = z0_v.shape[1]
    copies = []
    for c in range(3):
        for x in range(X):
            xb[c, x] = along * z0_v[c, x] + alpha1 * z1_v[c, x]
            rb[c, x] = r_v[c, x] - alpha1 * az_v[c, x] - a1b * y_v[c, x]
        for n, (src, dst) in enumerate(((xb, x_out), (rb, res_out))):
            copies.append(pltpu.make_async_copy(src.at[c], dst.at[c], sem.at[n, c]))
            copies[-1].start()
    for copy in copies:
        copy.wait()


def local(nw, nn, right_side, occupancy, region, coarse_inverse):
    _, X, Y, Z = right_side.shape
    ncr, NC = coarse_inverse.shape
    ND = nw * nn
    f32, i32 = jnp.float32, jnp.int32
    V = pltpu.VMEM
    field, pad, scal = (3, X, Y, Z), (3, X + 2, Y, Z), (X, Y, Z)
    scratch = [
        V(scal, i32), V(scal, i32), V((ncr, NC), f32),
        V((X + 2, Y, Z), f32), V((X + 1, Y, Z), f32),
        V(scal, f32), V(scal, f32), V(scal, f32), V(scal, f32), V(scal, f32), V(scal, f32),
        V(pad, f32), V(pad, f32),
        V((2, 3, X, Z), f32), V((2, 3, X, Z), f32),
        V((2, 2, Y, Z), i32), V((2, 2, X, Z), i32), V((2, 2, X, Z), i32),
        V((4, ncr, NC), f32),
        V((2, 2, 3, Y, Z), f32), V((2, 2, 3, Y, Z), f32),
        V((2, 2, 3, X, Z), f32), V((2, 2, 3, X, Z), f32),
        V((3, SUB, LANES), f32), V((3, ND, LANES), f32),
        pltpu.SemaphoreType.DMA((4,)),
        pltpu.SemaphoreType.DMA((5, 4)), pltpu.SemaphoreType.DMA((5, 4)),
        pltpu.SemaphoreType.DMA((3,)), pltpu.SemaphoreType.DMA((3,)),
    ]
    parts = pl.pallas_call(
        functools.partial(kernel, nw, nn),
        out_shape=(V(field, f32),) * 5 + (V((SUB, LANES), f32),),
        in_specs=[pl.BlockSpec(memory_space=pltpu.HBM)] * 4,
        out_specs=(pl.BlockSpec(memory_space=pltpu.VMEM),) * 6,
        scratch_shapes=scratch,
        compiler_params=pltpu.CompilerParams(collective_id=0, has_side_effects=True, vmem_limit_bytes=32 * 1024 * 1024),
    )(*[pltpu.with_memory_space_constraint(a, pltpu.HBM) for a in (right_side, occupancy, region, coarse_inverse)])
    return pl.pallas_call(
        finish,
        out_shape=(jax.ShapeDtypeStruct(field, f32),) * 2,
        in_specs=[pl.BlockSpec(memory_space=pltpu.VMEM)] * 6,
        out_specs=(pl.BlockSpec(memory_space=pltpu.HBM),) * 2,
        scratch_shapes=[V(field, f32), V(field, f32), pltpu.SemaphoreType.DMA((2, 3))],
        compiler_params=pltpu.CompilerParams(vmem_limit_bytes=16 * 1024 * 1024),
    )(*parts)


def solution(mesh):
    return jax.shard_map(
        functools.partial(local, mesh.shape["wide"], mesh.shape["narrow"]),
        mesh=mesh,
        in_specs=(
            P(None, "wide", "narrow", None),
            P("wide", "narrow", None),
            P("wide", "narrow", None),
            P(("wide", "narrow"), None),
        ),
        out_specs=(P(None, "wide", "narrow", None), P(None, "wide", "narrow", None)),
        check_vma=False,
    )
```
